32 devices in a mesh: nodes: 8 (over z, x), heads: 4 (over y, core).
Axes of the slice: x: 2, y: 2, z: 4, core: 2. Of those that a mesh axis runs over, the one named last changes fastest.
Arguments:
- nodes_in: bfloat16 [4096, 1024], P('nodes', 'heads'), may hold values from -6 to 6
- local_gain: float32 [1024], replicated, may hold values from 0.5 to 1.5
- neighbour_query_key_value: bfloat16 [3, 1024, 1024], P(None, None, 'heads'), may hold values from -0.25 to 0.25
- local_out: bfloat16 [1024, 1024], P('heads'), may hold values from -0.1875 to 0.1875
- global_gain: float32 [1024], replicated, may hold values from 0.5 to 1.5
- global_qkv: bfloat16 [3, 1024, 1024], P(None, None, 'heads'), may hold values from -0.1875 to 0.1875
- global_out: bfloat16 [1024, 1024], P('heads'), may hold values from -1.875 to 1.875
- feature_map: bfloat16 [16, 64, 128], P('heads'), may hold values from -5 to 5
- neighbour_count: int32 [32], P('nodes'), may hold values from 1 to 8
- neighbour_blocks: int32 [32, 8], P('nodes'), may hold values from 0 to 31, as said below
- metis_order: int32 [32], P('nodes'), may hold values from 0 to 31, as said below
- hashed_order: int32 [32], P('nodes'), may hold values from 0 to 31, as said below
Outputs:
- output: bfloat16 [4096, 1024], P('nodes', 'heads')
The draws below stay inside these ranges and needn't reach their ends.
Inputs may be any that keep to these rules, and one draw needn't show every extreme that they name: `neighbour_blocks`: entry 0 of block b's list is b itself; every entry lies within 2 blocks of the aligned group of 4 blocks that holds b, inside the graph; entries from neighbour_count on are unused; entries may repeat. `metis_order`: A permutation of the block ids. `hashed_order`: A permutation of the block ids. The blocks at the 4 METIS positions of aligned group g go to the aligned groups of 4 hashed positions numbered (g + k * 2) modulo 8 for k = 0 to 3, exactly 1 of them to each; which block goes to which of these groups, and to which position in it, is drawn.
All inputs are finite; a program needn't handle non-finite values.
Results may differ from the reference program's by a relative error of at most 0.015.
Values may be sent and summed in bfloat16 or wider, within the bound.
A program may use at most 64 MiB of HBM per device.

```python
import jax
import jax.numpy as jnp
from jax import lax

D = 1024
HEADS = 16
HD = 64
FEAT = 128
BLOCK = 128
MAXNB = 8
HALO_BLK = 2
BLK_DEV = 4
BLOCKS = 32
NODES = 4096
N_HEADS = 4


def draw_nodes_in(key, part):
    value_rows = jax.random.normal(jax.random.fold_in(key, 43), (NODES, D), jnp.float32)
    value_rows = jnp.clip(value_rows, -6.0, 6.0)
    return value_rows.astype(jnp.bfloat16)


def draw_neighbour_query_key_value(key, part):
    weights = jax.random.normal(jax.random.fold_in(key, 53), (3, D, D), jnp.float32) * D ** (-0.5)
    weights = jnp.clip(weights, -6.0 * D ** (-0.5), 6.0 * D ** (-0.5))
    return weights.astype(jnp.bfloat16)


def block_orders(key):
    base_key = jax.random.fold_in(key, 31)
    key_metis, key_lane, key_slot = jax.random.split(base_key, 3)
    groups = BLOCKS // BLK_DEV
    lane_count = min(BLK_DEV, groups)
    stride = max(1, groups // BLK_DEV)
    metis_ids = jax.random.permutation(key_metis, BLOCKS).astype(jnp.int32)
    offsets = jnp.arange(BLK_DEV, dtype=jnp.int32)[None, :]
    lane_scores = jax.random.randint(key_lane, (groups, BLK_DEV), 0, 1 << 20) * BLK_DEV + offsets
    lane_of = jnp.argsort(lane_scores, axis=1, stable=True).astype(jnp.int32)
    slot_scores = jax.random.randint(key_slot, (groups, BLK_DEV), 0, 1 << 20) * BLK_DEV + offsets
    slot_of = jnp.argsort(slot_scores, axis=1, stable=True).astype(jnp.int32)
    group_ids = jnp.arange(groups, dtype=jnp.int32)[:, None]
    owner_group = (group_ids + lane_of % lane_count * stride) % groups
    slot_index = slot_of[owner_group, lane_of]
    position = (owner_group * BLK_DEV + slot_index).reshape(-1)
    hashed = jnp.zeros((BLOCKS,), jnp.int32).at[position].set(metis_ids)
    return (metis_ids, hashed)


def draw_metis_order(key, part):
    return block_orders(key)[0]


def draw_hashed_order(key, part):
    return block_orders(key)[1]


def draw_neighbour_blocks(key, part):
    list_key = jax.random.fold_in(key, 17)
    block_ids = jnp.arange(BLOCKS, dtype=jnp.int32)
    group_start = block_ids // BLK_DEV * BLK_DEV
    lower = jnp.maximum(group_start - HALO_BLK, 0)
    upper = jnp.minimum(group_start + BLK_DEV + HALO_BLK, BLOCKS)
    raw_draws = jax.random.randint(list_key, (BLOCKS, MAXNB - 1), 0, 1 << 20)
    picked = lower[:, None] + raw_draws % (upper - lower)[:, None]
    return jnp.concatenate([block_ids[:, None], picked.astype(jnp.int32)], axis=1)


def with_ends(values, stream_key, least, high):
    longest = values.shape.index(max(values.shape))
    spots = []
    for shift in (0, 1):
        where = [jax.random.randint(jax.random.fold_in(stream_key, axis), (), 0, length) for axis, length in enumerate(values.shape)]
        where[longest] = (where[longest] + shift) % values.shape[longest]
        spots.append(tuple(where))
    return values.at[spots[0]].set(least).at[spots[1]].set(high)


def shard_levels(stream_key, shape, pieces, smallest, top_value):
    def one(dim, parts):
        heights = jax.random.uniform(jax.random.fold_in(jax.random.fold_in(stream_key, 6), dim), (parts,), jnp.float32, smallest / len(pieces), top_value / len(pieces))
        return jnp.repeat(jnp.exp(heights), shape[dim] // parts).reshape((-1,) + (1,) * (len(shape) - dim - 1))

    loudness = one(*pieces[0])
    for cut in pieces[1:]:
        loudness = loudness * one(*cut)
    return loudness


def normal_values(key, extent, spread, limit, pieces=(), kind=jnp.bfloat16):
    factor_of = shard_levels(key, extent, pieces, -0.22, 0.18) if pieces else 1.0
    values = jax.random.normal(key, extent, jnp.float32) * spread * factor_of
    return jnp.minimum(jnp.maximum(values, -limit), limit).astype(kind)


def setup_inputs(seed: int = 0) -> dict:
    streams_of = jax.random.split(jax.random.key(seed), 13)
    nodes_in = draw_nodes_in(jax.random.fold_in(streams_of[12], 71), 0)
    local_gain = jnp.clip(1.0 + 0.1 * jax.random.normal(streams_of[1], (D,), jnp.float32), 0.5, 1.5)
    neighbour_query_key_value = draw_neighbour_query_key_value(jax.random.fold_in(streams_of[12], 71), 0)
    local_out = normal_values(streams_of[3], (D, D), D ** -0.5, 0.1875, ((0, 4),))
    global_gain = jnp.clip(1.0 + 0.1 * jax.random.normal(streams_of[4], (D,), jnp.float32), 0.5, 1.5)
    global_qkv = normal_values(streams_of[5], (3, D, D), D ** -0.5, 0.1875, ((2, 4),))
    global_out = normal_values(streams_of[6], (D, D), (10.0 * D ** -0.5), 1.875, ((0, 4),))
    feature_map = normal_values(streams_of[7], (HEADS, HD, FEAT), 1.0, 5.0, ((0, 4),))
    neighbour_count = with_ends(jax.random.randint(streams_of[8], (BLOCKS,), 1, MAXNB + 1), jax.random.fold_in(streams_of[8], 1), 1, MAXNB).astype(jnp.int32)
    neighbour_blocks = draw_neighbour_blocks(jax.random.fold_in(streams_of[12], 71), 0)
    metis_order = draw_metis_order(jax.random.fold_in(streams_of[12], 71), 0)
    hashed_order = draw_hashed_order(jax.random.fold_in(streams_of[12], 71), 0)
    return {"nodes_in": nodes_in, "local_gain": local_gain, "neighbour_query_key_value": neighbour_query_key_value, "local_out": local_out, "global_gain": global_gain, "global_qkv": global_qkv, "global_out": global_out, "feature_map": feature_map, "neighbour_count": neighbour_count, "neighbour_blocks": neighbour_blocks, "metis_order": metis_order, "hashed_order": hashed_order}


EPSILON = 1e-06

def root_scale(row_data, gain_vector):
    as_float = row_data.astype(jnp.float32)
    mean_square = lax.optimization_barrier(jnp.mean(as_float * as_float, axis=-1, keepdims=True))
    return (as_float * lax.rsqrt(mean_square + EPSILON) * gain_vector).astype(jnp.bfloat16)

def project_three(rescaled_input, triple_weight):
    return [jnp.dot(rescaled_input, triple_weight[index], preferred_element_type=jnp.float32).astype(jnp.bfloat16) for index in range(3)]

def head_groups_sum(mixed_heads, out_weight):
    group_width = D // N_HEADS
    summed = jnp.zeros((mixed_heads.shape[0], D), jnp.float32)
    for group_index in range(N_HEADS):
        lower = group_index * group_width
        part_value = jnp.dot(mixed_heads[:, lower:lower + group_width], out_weight[lower:lower + group_width], preferred_element_type=jnp.float32).astype(jnp.bfloat16)
        part_value = lax.optimization_barrier(part_value)
        summed = summed + part_value.astype(jnp.float32)
    return summed

def local_attention(queries, keys_all, values_all, counts, neighbours):
    group_size = 4 if BLK_DEV % 4 == 0 else BLK_DEV
    query_groups = queries.reshape(BLOCKS // group_size, group_size, BLOCK, HEADS, HD)
    key_blocks = keys_all.reshape(BLOCKS, BLOCK, HEADS, HD)
    value_blocks = values_all.reshape(BLOCKS, BLOCK, HEADS, HD)
    slot_of_key = jnp.arange(MAXNB * BLOCK, dtype=jnp.int32) // BLOCK

    def one_group(inputs):
        query_group, index_group, count_group = inputs
        keys_sel = key_blocks[index_group].reshape(group_size, MAXNB * BLOCK, HEADS, HD)
        values_sel = value_blocks[index_group].reshape(group_size, MAXNB * BLOCK, HEADS, HD)
        scores = jnp.einsum('gqhd,gkhd->ghqk', query_group.astype(jnp.float32), keys_sel.astype(jnp.float32)) * HD ** (-0.5)
        live = slot_of_key[None, :] < count_group[:, None]
        scores = jnp.where(live[:, None, None, :], scores, -jnp.inf)
        row_max = lax.optimization_barrier(jnp.max(scores, axis=-1, keepdims=True))
        expo = jnp.exp(scores - row_max)
        totals = lax.optimization_barrier(jnp.sum(expo, axis=-1))
        local_weights = expo.astype(jnp.bfloat16)
        mixed_heads = jnp.einsum('ghqk,gkhd->gqhd', local_weights.astype(jnp.float32), values_sel.astype(jnp.float32))
        mixed_heads = mixed_heads / jnp.transpose(totals, (0, 2, 1))[..., None]
        return mixed_heads.astype(jnp.bfloat16)
    mixed_all = lax.map(one_group, (query_groups, neighbours.reshape(BLOCKS // group_size, group_size, MAXNB), counts.reshape(BLOCKS // group_size, group_size)))
    return mixed_all.reshape(NODES, D)

def feature_maps(row_data, feature_map):
    angles = jnp.einsum('nhd,hdf->nhf', row_data.reshape(NODES, HEADS, HD).astype(jnp.float32), feature_map.astype(jnp.float32)) * HD ** (-0.5)
    return (jax.nn.elu(angles) + 1.0).astype(jnp.bfloat16)

def reference(nodes_in, local_gain, neighbour_query_key_value, local_out, global_gain, global_qkv, global_out, feature_map, neighbour_count, neighbour_blocks, metis_order, hashed_order):
    local_rescaled = root_scale(nodes_in, local_gain)
    queries, keys_all, values_all = project_three(local_rescaled, neighbour_query_key_value)
    local_mixed = local_attention(queries, keys_all, values_all, neighbour_count, neighbour_blocks)
    hidden = (nodes_in.astype(jnp.float32) + head_groups_sum(local_mixed, local_out)).astype(jnp.bfloat16)
    normed_global = root_scale(hidden, global_gain)
    global_queries, global_keys, global_values = project_three(normed_global, global_qkv)
    phi_query = feature_maps(global_queries, feature_map).astype(jnp.float32)
    phi_key = feature_maps(global_keys, feature_map).astype(jnp.float32)
    summary = jnp.einsum('nhf,nhd->hfd', phi_key, global_values.reshape(NODES, HEADS, HD).astype(jnp.float32))
    key_total = lax.optimization_barrier(jnp.sum(phi_key, axis=0))
    numerator = jnp.einsum('nhf,hfd->nhd', phi_query, summary, precision=lax.Precision.HIGHEST)
    denominator = jnp.einsum('nhf,hf->nh', phi_query, key_total, precision=lax.Precision.HIGHEST)
    global_mixed = (numerator / denominator[..., None]).astype(jnp.bfloat16).reshape(NODES, D)
    metis_out = (hidden.astype(jnp.float32) + head_groups_sum(global_mixed, global_out)).astype(jnp.bfloat16)
    position = jnp.zeros((BLOCKS,), jnp.int32).at[metis_order].set(jnp.arange(BLOCKS, dtype=jnp.int32))
    source = position[hashed_order]
    return metis_out.reshape(BLOCKS, BLOCK, D)[source].reshape(NODES, D)
```

```python
import functools

import jax
import jax.numpy as jnp
from jax import lax
from jax.experimental import pallas as pl
from jax.experimental.pallas import tpu as pltpu
from jax.sharding import PartitionSpec as P

HD = 64
BLOCK = 128
EPSILON = 1e-06
MESH = pl.DeviceIdType.MESH
BF = jnp.bfloat16
F32 = jnp.float32


def dot(a, b):
    return jnp.dot(a, b, preferred_element_type=F32)


def kernel(
    N, B, SLOTS,
    x_ref, lg_ref, w1_hbm, lo_hbm, gg_ref, w2_hbm, go_hbm, fm_ref, cnt_ref, nb_ref, ids_ref,
    out_ref,
    w1, lo, w2, go, XE, KX, VX, Q, FMB, IDR, LP, LR, LS, LY, HID, PQ, SA, SB, RR, AG,
    QL, HL, GP, GR, GS, GOWN, GY, FB, RB,
    wsem, xcs, xcr, xys, xyr, xfs, xfr, has, har, ids_s, ids_r,
    lcs, lcr, lys, lyr, lhs, lhr, rss, rsr, ags, agr, gcs, gcr, gys, gyr, gzs, gzr,
):
    me = lax.axis_index("nodes")
    h = lax.axis_index("heads")
    y, c = h // 2, h % 2
    pc = h + 1 - 2 * c
    py = h + 2 - 4 * y
    HALF = x_ref.shape[0] // 2
    W = x_ref.shape[1]
    D = 4 * W
    L = 4
    stride = N // L
    NP = W // 128

    def rcopy(src, dst, ss, rs, n, hh):
        return pltpu.make_async_remote_copy(
            src_ref=src, dst_ref=dst, send_sem=ss, recv_sem=rs,
            device_id=(n, hh), device_id_type=MESH)

    weights = [pltpu.make_async_copy(s, d, wsem.at[i])
               for i, (s, d) in enumerate(((w1_hbm, w1), (lo_hbm, lo), (w2_hbm, w2), (go_hbm, go)))]
    for wcopy in weights:
        wcopy.start()

    barrier = pltpu.get_barrier_semaphore()
    for hh in (pc, py):
        pl.semaphore_signal(barrier, inc=1, device_id=(me, hh), device_id_type=MESH)

    @pl.loop(1, N)
    def _(d):
        pl.semaphore_signal(barrier, inc=1, device_id=(lax.rem(me + d, N), h), device_id_type=MESH)

    XE[c, y, 0] = x_ref[0:HALF]
    XE[c, y, 1] = x_ref[HALF:2 * HALF]
    FMB[...] = jnp.zeros_like(FMB)
    for p in range(NP):
        FMB[p, 0:HD, 0:128] = fm_ref[2 * p]
        FMB[p, HD:2 * HD, 128:256] = fm_ref[2 * p + 1]
    IDR[0] = ids_ref[...]

    @pl.when(me == 0)
    def _():
        XE[c, y, 2] = jnp.zeros((HALF, W), BF)

    @pl.when(me == N - 1)
    def _():
        XE[c, y, 3] = jnp.zeros((HALF, W), BF)

    pl.semaphore_wait(barrier, N + 1)

    def piece(k):
        return x_ref.at[pl.ds(k * HALF, HALF)] if k < 2 else XE.at[c, y, k]

    def x_core(k):
        return rcopy(piece(k), XE.at[c, y, k], xcs.at[k], xcr.at[k], me, pc)

    def x_y(k):
        return rcopy(piece(k), XE.at[c, y, k], xys.at[k], xyr.at[k], me, py)

    def x_fwd(k):
        return rcopy(XE.at[c, 1 - y, k], XE.at[c, 1 - y, k], xfs.at[k], xfr.at[k], me, pc)

    up, down = lax.rem(me + 1, N), lax.rem(me + N - 1, N)
    halo_up = rcopy(piece(1), XE.at[c, y, 2], has.at[0], har.at[0], up, h)
    halo_down = rcopy(piece(0), XE.at[c, y, 3], has.at[1], har.at[1], down, h)

    x_y(0).start()
    x_y(1).start()

    @pl.when(me < N - 1)
    def _():
        halo_up.start()

    @pl.when(me > 0)
    def _():
        halo_down.start()

    x_core(0).start()
    x_core(1).start()

    def id_copy(k):
        return rcopy(ids_ref, IDR.at[k], ids_s.at[k], ids_r.at[k], lax.rem(me + k * stride, N), h)

    for k in range(1, L):
        id_copy(k).start()

    x_y(0).wait_recv()
    x_fwd(0).start()

    @pl.when(me > 0)
    def _():
        halo_up.wait_recv()

    x_y(2).start()
    x_core(2).start()
    x_y(1).wait_recv()
    x_fwd(1).start()

    @pl.when(me < N - 1)
    def _():
        halo_down.wait_recv()

    x_y(3).start()
    x_core(3).start()

    def normed(parts, gain_ref):
        floats = [part.astype(F32) for part in parts]
        total = sum(jnp.sum(f * f, axis=-1, keepdims=True) for f in floats)
        scale = lax.rsqrt(total * (1.0 / D) + EPSILON)
        return jnp.concatenate(
            [(f * scale * gain_ref[:, s * W:(s + 1) * W]).astype(BF) for s, f in enumerate(floats)], axis=1)

    def project(k, with_queries):
        x_core(k).wait_recv()
        x_fwd(k).wait_recv()
        rows = normed([XE[s % 2, s // 2, k] for s in range(4)], lg_ref)
        first = (2, 4, 0, 6)[k]
        if with_queries:
            q = (dot(rows, w1[0]).astype(BF).astype(F32) * HD ** (-0.5)).astype(BF)
            Q[2 * k:2 * k + 2] = q.reshape(2, BLOCK, W)
        KX[first:first + 2] = dot(rows, w1[1]).astype(BF).reshape(2, BLOCK, W)
        VX[first:first + 2] = dot(rows, w1[2]).astype(BF).reshape(2, BLOCK, W)

    weights[0].wait()
    project(0, True)
    project(1, True)
    x_y(2).wait_recv()
    x_fwd(2).start()
    x_y(3).wait_recv()
    x_fwd(3).start()
    project(2, False)
    project(3, False)
    weights[1].wait()

    low = lax.broadcasted_iota(jnp.int32, (BLOCK, 128), 1) < HD
    slot_of = lax.broadcasted_iota(jnp.int32, (1, SLOTS * BLOCK), 1) // BLOCK

    def l_core(b):
        return rcopy(LP.at[b, 1 - c], LR.at[b], lcs.at[b], lcr.at[b], me, pc)

    def l_y(b):
        return rcopy(LS.at[b], LY.at[b], lys.at[b], lyr.at[b], me, py)

    def l_hid(b):
        return rcopy(HID.at[b, c], HID.at[b, c], lhs.at[b], lhr.at[b], me, pc)

    def l_reduce(b):
        l_core(b).wait_recv()
        LS[b] = (LP[b, c].astype(F32) + LR[b].astype(F32)).astype(BF)
        l_y(b).start()

    @pl.loop(0, B)
    def _(b):
        picks = [jnp.clip(nb_ref[b, s] - (me * B - 2), 0, 2 * B - 1) for s in range(SLOTS)]
        live = slot_of < cnt_ref[b]
        mixed = []
        for p in range(NP):
            cols = slice(p * 128, (p + 1) * 128)
            q = Q[b, :, cols].astype(F32)
            both = jnp.concatenate([jnp.where(low, q, 0.0), jnp.where(low, 0.0, q)], axis=0).astype(BF)
            keys = jnp.concatenate([KX[i, :, cols] for i in picks], axis=0)
            vals = jnp.concatenate([VX[i, :, cols] for i in picks], axis=0)
            scores = lax.dot_general(both, keys, (((1,), (1,)), ((), ())), preferred_element_type=F32)
            scores = jnp.where(live, scores, -1e30)
            expo = jnp.exp(scores - jnp.max(scores, axis=-1, keepdims=True))
            totals = jnp.sum(expo, axis=-1, keepdims=True)
            o = dot(expo.astype(BF), vals) / totals
            mixed.append(jnp.where(low, o[:BLOCK], o[BLOCK:]).astype(BF))
        part = dot(jnp.concatenate(mixed, axis=1), lo[...]).astype(BF)
        for s in range(4):
            LP[b, s % 2, s // 2] = part[:, s * W:(s + 1) * W]
        l_core(b).start()

        @pl.when(b > 0)
        def _():
            l_reduce(b - 1)

    l_reduce(B - 1)
    weights[2].wait()
    SA[...] = jnp.zeros_like(SA)

    def features(rows, p):
        u = dot(rows[:, p * 128:(p + 1) * 128], FMB[p]) * HD ** (-0.5)
        return jnp.where(u > 0, u + 1.0, jnp.exp(jnp.minimum(u, 0.0))).astype(BF)

    def global_block(b):
        l_hid(b).wait_recv()
        rows = normed([HID[b, s % 2, s // 2] for s in range(4)], gg_ref)
        gq = dot(rows, w2[0]).astype(BF)
        gk = dot(rows, w2[1]).astype(BF)
        gv = dot(rows, w2[2]).astype(BF).astype(F32)
        for p in range(NP):
            PQ[b, :, p * 256:(p + 1) * 256] = features(gq, p)
            fk = features(gk, p)
            v = gv[:, p * 128:(p + 1) * 128]
            for side in range(2):
                ext = (jnp.where(low, v, 1.0) if side == 0 else jnp.where(low, 1.0, v)).astype(BF)
                head = 2 * p + side
                SA[head * 128:(head + 1) * 128] += lax.dot_general(
                    fk[:, side * 128:(side + 1) * 128], ext, (((0,), (0,)), ((), ())),
                    preferred_element_type=F32)

    @pl.loop(0, B)
    def _(b):
        l_y(b).wait_recv()
        for yy in range(2):
            own = XE[c, yy, b // 2, pl.ds(pl.multiple_of((b % 2) * BLOCK, BLOCK), BLOCK)].astype(F32)
            HID[b, c, yy] = (own + (LS[b, yy].astype(F32) + LY[b, yy].astype(F32))).astype(BF)
        l_hid(b).start()

        @pl.when(b > 0)
        def _():
            global_block(b - 1)

    global_block(B - 1)

    SB[...] = SA[...].reshape(SB.shape).astype(BF)

    def rs_copy(d):
        to = lax.rem(me + d, N)
        return rcopy(SB.at[to], RR.at[d], rss.at[d], rsr.at[d], to, h)

    def ag_copy(d):
        to = lax.rem(me + d, N)
        return rcopy(AG.at[me], AG.at[me], ags.at[d], agr.at[d], to, h)

    def ag_arrival(d):
        origin = lax.rem(me + N - d, N)
        return rcopy(AG.at[origin], AG.at[origin], ags.at[d], agr.at[d], lax.rem(me + d, N), h)

    @pl.loop(1, N)
    def _(d):
        rs_copy(d).start()

    for k in range(1, L):
        id_copy(k).wait_recv()

    def weight(id_row, rows):
        same = jnp.zeros((1, 128), F32)
        for j in range(B):
            same = same + jnp.where(id_row == rows[j:j + 1], 1.0, 0.0)
        return same

    def wide(w, width):
        return jnp.concatenate([w] * (width // 128), axis=1)

    for k in range(L):
        hashed = IDR[(L - k) % L][B:2 * B]
        q_sum, h_sum = None, None
        for i in range(B):
            w = weight(ids_ref[i:i + 1], hashed)
            qt = wide(w, 2 * W) * PQ[i].astype(F32)
            ht = wide(w, W) * HID[i, c, y].astype(F32)
            q_sum = qt if q_sum is None else q_sum + qt
            h_sum = ht if h_sum is None else h_sum + ht
        QL[k] = q_sum.astype(BF)
        HL[k] = h_sum

    RR[0] = SB[me]

    @pl.loop(1, N)
    def _(d):
        rs_copy(d).wait_recv()

    AG[me] = jnp.sum(RR[...].astype(F32), axis=0).astype(BF)

    @pl.loop(1, N)
    def _(d):
        ag_copy(d).start()

    weights[3].wait()

    @pl.loop(1, N)
    def _(d):
        ag_arrival(d).wait_recv()

    SA[...] = AG[...].astype(F32).reshape(SA.shape)

    def g_core(k):
        return rcopy(GP.at[k, 1 - c], GR.at[k], gcs.at[k], gcr.at[k], me, pc)

    def g_y(k):
        return rcopy(GS.at[k], GY.at[k], gys.at[k], gyr.at[k], me, py)

    def g_z(k):
        return rcopy(FB.at[k], RB.at[k], gzs.at[k], gzr.at[k], lax.rem(me + k * stride, N), h)

    def mix(k):
        mixed = []
        for p in range(NP):
            r = []
            for side in range(2):
                head = 2 * p + side
                r.append(dot(QL[k, :, head * 128:(head + 1) * 128],
                             SA[head * 128:(head + 1) * 128].astype(BF)))
            top = jnp.where(low, r[0], r[1])
            below = pltpu.roll(jnp.where(low, r[1], r[0]), HD, 1)
            mixed.append((top / below).astype(BF))
        part = dot(jnp.concatenate(mixed, axis=1), go[...]).astype(BF)
        for s in range(4):
            GP[k, s % 2, s // 2] = part[:, s * W:(s + 1) * W]
        g_core(k).start()

    def g_reduce(k):
        g_core(k).wait_recv()
        GS[k] = (GP[k, c, 1 - y].astype(F32) + GR[k, 1 - y].astype(F32)).astype(BF)
        g_y(k).start()
        GOWN[k] = GP[k, c, y].astype(F32) + GR[k, y].astype(F32)

    order = (2, 1, 3, 0)
    for t, k in enumerate(order):
        mix(k)
        if t > 0:
            g_reduce(order[t - 1])
    g_reduce(order[-1])
    for k in order:
        g_y(k).wait_recv()
        final = (HL[k] + (GOWN[k] + GY[k].astype(F32))).astype(BF)
        if k:
            FB[k] = final
            g_z(k).start()
        else:
            RB[0] = final
    for k in range(1, L):
        g_z(k).wait_recv()
    for j in range(B):
        acc = None
        for k in range(L):
            w = weight(ids_ref[B + j:B + j + 1], IDR[k][0:B])
            term = wide(w, W) * RB[k].astype(F32)
            acc = term if acc is None else acc + term
        out_ref[j * BLOCK:(j + 1) * BLOCK] = acc.astype(BF)

    for k in range(4):
        x_y(k).wait_send()
        x_core(k).wait_send()
        x_fwd(k).wait_send()

    @pl.when(me < N - 1)
    def _():
        halo_up.wait_send()

    @pl.when(me > 0)
    def _():
        halo_down.wait_send()

    for k in range(1, L):
        id_copy(k).wait_send()
        g_z(k).wait_send()
    for b in range(B):
        l_core(b).wait_send()
        l_y(b).wait_send()
        l_hid(b).wait_send()
        g_core(b).wait_send()
        g_y(b).wait_send()

    @pl.loop(1, N)
    def _(d):
        rs_copy(d).wait_send()
        ag_copy(d).wait_send()


def body(
    N, nodes_in, local_gain, w1, local_out, global_gain, w2, global_out, feature_map,
    neighbour_count, neighbour_blocks, metis_order, hashed_order,
):
    rows, W = nodes_in.shape
    B = metis_order.shape[0]
    SLOTS = neighbour_blocks.shape[1]
    D = w1.shape[1]
    SR = feature_map.shape[0] * feature_map.shape[2]
    ids = jnp.concatenate([metis_order, hashed_order])
    ids = jnp.broadcast_to(ids[:, None], (2 * B, 128))
    vm = pl.BlockSpec(memory_space=pltpu.VMEM)
    sm = pl.BlockSpec(memory_space=pltpu.SMEM)
    hb = pl.BlockSpec(memory_space=pl.ANY)

    def V(*shape, dtype=BF):
        return pltpu.VMEM(shape, dtype)

    half = rows // 2
    S = pltpu.SemaphoreType.DMA
    scratch = [
        V(3, D, W), V(W, D), V(3, D, W), V(W, D),
        V(2, 2, 4, half, W), V(2 * B, BLOCK, W), V(2 * B, BLOCK, W), V(B, BLOCK, W),
        V(W // 128, 128, 256), V(4, 2 * B, 128, dtype=jnp.int32),
        V(B, 2, 2, BLOCK, W), V(B, 2, BLOCK, W), V(B, 2, BLOCK, W), V(B, 2, BLOCK, W),
        V(B, 2, 2, BLOCK, W), V(B, BLOCK, 2 * W), V(SR, 128, dtype=F32),
        V(N, SR // N, 128), V(N, SR // N, 128), V(N, SR // N, 128),
        V(4, BLOCK, 2 * W), V(4, BLOCK, W, dtype=F32),
        V(4, 2, 2, BLOCK, W), V(4, 2, BLOCK, W), V(4, BLOCK, W), V(4, BLOCK, W, dtype=F32),
        V(4, BLOCK, W), V(4, BLOCK, W), V(4, BLOCK, W),
        S((4,)),
    ] + [S((4,))] * 6 + [S((2,))] * 2 + [S((4,))] * 2 + [S((4,))] * 6 + [S((N,))] * 4 + [S((4,))] * 6
    return pl.pallas_call(
        functools.partial(kernel, N, B, SLOTS),
        out_shape=jax.ShapeDtypeStruct((rows, W), BF),
        in_specs=[vm, vm, hb, hb, vm, hb, hb, vm, sm, sm, vm],
        out_specs=vm,
        scratch_shapes=scratch,
        compiler_params=pltpu.CompilerParams(
            collective_id=0, has_side_effects=True, vmem_limit_bytes=48 * 1024 * 1024),
        name="graph_pair",
    )(nodes_in, local_gain.reshape(1, D), w1, local_out, global_gain.reshape(1, D), w2, global_out,
      feature_map, neighbour_count, neighbour_blocks, ids)


def solution(mesh):
    in_specs = (
        P("nodes", "heads"), P(), P(None, None, "heads"), P("heads", None), P(),
        P(None, None, "heads"), P("heads", None), P("heads", None, None),
        P("nodes"), P("nodes", None), P("nodes"), P("nodes"),
    )
    return jax.shard_map(
        functools.partial(body, mesh.shape["nodes"]), mesh=mesh, in_specs=in_specs,
        out_specs=P("nodes", "heads"), check_vma=False)
```

```python
import functools

import jax
import jax.numpy as jnp
from jax import lax
from jax.experimental import pallas as pl
from jax.experimental.pallas import tpu as pltpu
from jax.sharding import PartitionSpec as P

HD = 64
BLOCK = 128
EPSILON = 1e-06
MESH = pl.DeviceIdType.MESH
BF = jnp.bfloat16
F32 = jnp.float32


def dot(a, b):
    return jnp.dot(a, b, preferred_element_type=F32)


def kernel(
    N, B, SLOTS,
    x_hbm, lg_hbm, w1_hbm, lo_hbm, gg_hbm, w2_hbm, go_hbm, fm_hbm, cnt_hbm, nb_hbm, metis_hbm, hashed_hbm,
    out_ref,
    x_ref, lg_ref, gg_ref, fm_ref, cnt_ref, nb_ref, metis_ref, hashed_ref, ids_ref, OF, w1, lo, w2, go, XE, KX, VX, Q, FMB, IDR, LP, LR, LS, LY, HID, PQ, SA, SB, RR, AG,
    QL, HL, GP, GR, GS, GOWN, GY, FB, RB,
    isem, wsem, xcs, xcr, xys, xyr, xfs, xfr, has, har, ids_s, ids_r,
    lcs, lcr, lys, lyr, lhs, lhr, rss, rsr, ags, agr, gcs, gcr, gys, gyr, gzs, gzr,
):
    me = lax.axis_index("nodes")
    h = lax.axis_index("heads")
    y, c = h // 2, h % 2
    pc = h + 1 - 2 * c
    py = h + 2 - 4 * y
    HALF = x_ref.shape[0] // 2
    W = x_ref.shape[1]
    D = 4 * W
    L = 4
    stride = N // L
    NP = W // 128

    def rcopy(src, dst, ss, rs, n, hh):
        return pltpu.make_async_remote_copy(
            src_ref=src, dst_ref=dst, send_sem=ss, recv_sem=rs,
            device_id=(n, hh), device_id_type=MESH)

    barrier = pltpu.get_barrier_semaphore()

    @pl.loop(1, N)
    def _(d):
        pl.semaphore_signal(barrier, inc=1, device_id=(lax.rem(me + d, N), h), device_id_type=MESH)

    for hh in (pc, py):
        pl.semaphore_signal(barrier, inc=1, device_id=(me, hh), device_id_type=MESH)

    small = [pltpu.make_async_copy(s, d, isem.at[i])
             for i, (s, d) in enumerate((
                 (x_hbm, x_ref), (metis_hbm, metis_ref), (hashed_hbm, hashed_ref), (fm_hbm, fm_ref),
                 (lg_hbm, lg_ref), (gg_hbm, gg_ref), (cnt_hbm, cnt_ref), (nb_hbm, nb_ref)))]
    weights = [pltpu.make_async_copy(s, d, wsem.at[i])
               for i, (s, d) in enumerate(((w1_hbm, w1), (lo_hbm, lo), (w2_hbm, w2), (go_hbm, go)))]
    for each in small + weights:
        each.start()
    FMB[...] = jnp.zeros_like(FMB)
    for each in small:
        each.wait()
    XE[c, y, 0] = x_ref[0:HALF]
    XE[c, y, 1] = x_ref[HALF:2 * HALF]
    for p in range(NP):
        FMB[p, 0:HD, 0:128] = fm_ref[2 * p]
        FMB[p, HD:2 * HD, 128:256] = fm_ref[2 * p + 1]
    for j in range(B):
        ids_ref[j:j + 1] = jnp.full((1, 128), metis_ref[j], jnp.int32)
        ids_ref[B + j:B + j + 1] = jnp.full((1, 128), hashed_ref[j], jnp.int32)
    IDR[0] = ids_ref[...]

    @pl.when(me == 0)
    def _():
        XE[c, y, 2] = jnp.zeros((HALF, W), BF)

    @pl.when(me == N - 1)
    def _():
        XE[c, 0, 3] = jnp.zeros((HALF, W), BF)
        XE[c, 1, 3] = jnp.zeros((HALF, W), BF)

    pl.semaphore_wait(barrier, N + 1)

    def piece(k):
        return x_ref.at[pl.ds(k * HALF, HALF)] if k < 2 else XE.at[c, y, k]

    def x_core(k):
        return rcopy(piece(k), XE.at[c, y, k], xcs.at[k], xcr.at[k], me, pc)

    def x_y(k):
        return rcopy(piece(k), XE.at[c, y, k], xys.at[k], xyr.at[k], me, py)

    def x_fwd(k):
        return rcopy(XE.at[c, 1 - y, k], XE.at[c, 1 - y, k], xfs.at[k], xfr.at[k], me, pc)

    up, down = lax.rem(me + 1, N), lax.rem(me + N - 1, N)
    halo_up = rcopy(piece(1), XE.at[c, y, 2], has.at[0], har.at[0], up, h)
    halo_down = rcopy(piece(0), XE.at[c, y, 3], has.at[1], har.at[1], down, h)

    halo_far = rcopy(XE.at[c, 1 - y, 0], XE.at[c, 1 - y, 3], has.at[2], har.at[2], down, h)

    x_y(0).start()
    x_y(1).start()

    @pl.when(me < N - 1)
    def _():
        halo_up.start()

    @pl.when(me > 0)
    def _():
        halo_down.start()

    x_core(0).start()
    x_core(1).start()

    def id_copy(k):
        return rcopy(ids_ref, IDR.at[k], ids_s.at[k], ids_r.at[k], lax.rem(me + k * stride, N), h)

    for k in range(1, L):
        id_copy(k).start()

    x_y(0).wait_recv()
    x_fwd(0).start()

    @pl.when(me > 0)
    def _():
        halo_far.start()

    @pl.when(me > 0)
    def _():
        halo_up.wait_recv()

    x_y(2).start()
    x_core(2).start()
    x_y(1).wait_recv()
    x_fwd(1).start()

    @pl.when(me < N - 1)
    def _():
        halo_down.wait_recv()

    x_core(3).start()

    def normed(parts, gain_ref):
        floats = [part.astype(F32) for part in parts]
        total = sum(jnp.sum(f * f, axis=-1, keepdims=True) for f in floats)
        scale = lax.rsqrt(total * (1.0 / D) + EPSILON)
        return jnp.concatenate(
            [(f * scale * gain_ref[:, s * W:(s + 1) * W]).astype(BF) for s, f in enumerate(floats)], axis=1)

    def project(k, with_queries):
        x_core(k).wait_recv()
        x_fwd(k).wait_recv()
        rows = normed([XE[s % 2, s // 2, k] for s in range(4)], lg_ref)
        first = (2, 4, 0, 6)[k]
        if with_queries:
            q = (dot(rows, w1[0]).astype(BF).astype(F32) * HD ** (-0.5)).astype(BF)
            Q[2 * k:2 * k + 2] = q.reshape(2, BLOCK, W)
        KX[first:first + 2] = dot(rows, w1[1]).astype(BF).reshape(2, BLOCK, W)
        VX[first:first + 2] = dot(rows, w1[2]).astype(BF).reshape(2, BLOCK, W)

    weights[0].wait()
    project(0, True)
    project(1, True)
    x_y(2).wait_recv()
    x_fwd(2).start()

    @pl.when(me < N - 1)
    def _():
        halo_far.wait_recv()

    x_fwd(3).start()
    project(2, False)
    project(3, False)
    weights[1].wait()

    low = lax.broadcasted_iota(jnp.int32, (BLOCK, 128), 1) < HD
    slot_of = lax.broadcasted_iota(jnp.int32, (1, SLOTS * BLOCK), 1) // BLOCK

    def l_core(b):
        return rcopy(LP.at[b, 1 - c], LR.at[b], lcs.at[b], lcr.at[b], me, pc)

    def l_y(b):
        return rcopy(LS.at[b], LY.at[b], lys.at[b], lyr.at[b], me, py)

    def l_hid(b):
        return rcopy(HID.at[b, c], HID.at[b, c], lhs.at[b], lhr.at[b], me, pc)

    def l_reduce(b):
        l_core(b).wait_recv()
        LS[b] = (LP[b, c].astype(F32) + LR[b].astype(F32)).astype(BF)
        l_y(b).start()

    @pl.loop(0, B)
    def _(b):
        picks = [jnp.clip(nb_ref[b, s] - (me * B - 2), 0, 2 * B - 1) for s in range(SLOTS)]
        live = slot_of < cnt_ref[b]
        mixed = []
        for p in range(NP):
            cols = slice(p * 128, (p + 1) * 128)
            q = Q[b, :, cols].astype(F32)
            both = jnp.concatenate([jnp.where(low, q, 0.0), jnp.where(low, 0.0, q)], axis=0).astype(BF)
            keys = jnp.concatenate([KX[i, :, cols] for i in picks], axis=0)
            vals = jnp.concatenate([VX[i, :, cols] for i in picks], axis=0)
            scores = lax.dot_general(both, keys, (((1,), (1,)), ((), ())), preferred_element_type=F32)
            scores = jnp.where(live, scores, -1e30)
            expo = jnp.exp(scores - jnp.max(scores, axis=-1, keepdims=True))
            totals = jnp.sum(expo, axis=-1, keepdims=True)
            o = dot(expo.astype(BF), vals) / totals
            mixed.append(jnp.where(low, o[:BLOCK], o[BLOCK:]).astype(BF))
        part = dot(jnp.concatenate(mixed, axis=1), lo[...]).astype(BF)
        for s in range(4):
            LP[b, s % 2, s // 2] = part[:, s * W:(s + 1) * W]
        l_core(b).start()

        @pl.when(b > 0)
        def _():
            l_reduce(b - 1)

    l_reduce(B - 1)
    weights[2].wait()
    SA[...] = jnp.zeros_like(SA)

    def features(rows, p):
        u = dot(rows[:, p * 128:(p + 1) * 128], FMB[p]) * HD ** (-0.5)
        return jnp.where(u > 0, u + 1.0, jnp.exp(jnp.minimum(u, 0.0))).astype(BF)

    def global_queries(b, rows):
        gq = dot(rows, w2[0]).astype(BF)
        for p in range(NP):
            PQ[b, :, p * 256:(p + 1) * 256] = features(gq, p)

    def global_block(b):
        l_hid(b).wait_recv()
        rows = normed([HID[b, s % 2, s // 2] for s in range(4)], gg_ref)
        gk = dot(rows, w2[1]).astype(BF)
        gv = dot(rows, w2[2]).astype(BF).astype(F32)
        for p in range(NP):
            fk = features(gk, p)
            v = gv[:, p * 128:(p + 1) * 128]
            for side in range(2):
                ext = (jnp.where(low, v, 1.0) if side == 0 else jnp.where(low, 1.0, v)).astype(BF)
                head = 2 * p + side
                SA[head * 128:(head + 1) * 128] += lax.dot_general(
                    fk[:, side * 128:(side + 1) * 128], ext, (((0,), (0,)), ((), ())),
                    preferred_element_type=F32)
        return rows

    @pl.loop(0, B)
    def _(b):
        l_y(b).wait_recv()
        for yy in range(2):
            own = XE[c, yy, b // 2, pl.ds(pl.multiple_of((b % 2) * BLOCK, BLOCK), BLOCK)].astype(F32)
            HID[b, c, yy] = (own + (LS[b, yy].astype(F32) + LY[b, yy].astype(F32))).astype(BF)
        l_hid(b).start()

        @pl.when(b > 0)
        def _():
            global_queries(b - 1, global_block(b - 1))

    last_rows = global_block(B - 1)

    SB[...] = SA[...].reshape(SB.shape).astype(BF)

    def rs_copy(d):
        to = lax.rem(me + d, N)
        return rcopy(SB.at[to], RR.at[d], rss.at[d], rsr.at[d], to, h)

    def ag_copy(d):
        to = lax.rem(me + d, N)
        return rcopy(AG.at[me], AG.at[me], ags.at[d], agr.at[d], to, h)

    def ag_arrival(d):
        origin = lax.rem(me + N - d, N)
        return rcopy(AG.at[origin], AG.at[origin], ags.at[d], agr.at[d], lax.rem(me + d, N), h)

    @pl.loop(1, N)
    def _(d):
        rs_copy(d).start()

    global_queries(B - 1, last_rows)
    for k in range(1, L):
        id_copy(k).wait_recv()

    def weight(id_row, rows):
        same = jnp.zeros((1, 128), F32)
        for j in range(B):
            same = same + jnp.where(id_row == rows[j:j + 1], 1.0, 0.0)
        return same

    def wide(w, width):
        return jnp.concatenate([w] * (width // 128), axis=1)

    for k in range(L):
        hashed = IDR[(L - k) % L][B:2 * B]
        q_sum, h_sum = None, None
        for i in range(B):
            w = weight(ids_ref[i:i + 1], hashed)
            qt = wide(w, 2 * W) * PQ[i].astype(F32)
            ht = wide(w, W) * HID[i, c, y].astype(F32)
            q_sum = qt if q_sum is None else q_sum + qt
            h_sum = ht if h_sum is None else h_sum + ht
        QL[k] = q_sum.astype(BF)
        HL[k] = h_sum

    RR[0] = SB[me]

    @pl.loop(1, N)
    def _(d):
        rs_copy(d).wait_recv()

    AG[me] = jnp.sum(RR[...].astype(F32), axis=0).astype(BF)

    @pl.loop(1, N)
    def _(d):
        ag_copy(d).start()

    weights[3].wait()

    @pl.loop(1, N)
    def _(d):
        ag_arrival(d).wait_recv()

    SA[...] = AG[...].astype(F32).reshape(SA.shape)

    def g_core(k):
        return rcopy(GP.at[k, 1 - c], GR.at[k], gcs.at[k], gcr.at[k], me, pc)

    def g_y(k):
        return rcopy(GS.at[k], GY.at[k], gys.at[k], gyr.at[k], me, py)

    def g_z(k):
        return rcopy(FB.at[k], RB.at[k], gzs.at[k], gzr.at[k], lax.rem(me + k * stride, N), h)

    def mix(k):
        mixed = []
        for p in range(NP):
            r = []
            for side in range(2):
                head = 2 * p + side
                r.append(dot(QL[k, :, head * 128:(head + 1) * 128],
                             SA[head * 128:(head + 1) * 128].astype(BF)))
            top = jnp.where(low, r[0], r[1])
            below = pltpu.roll(jnp.where(low, r[1], r[0]), HD, 1)
            mixed.append((top / below).astype(BF))
        part = dot(jnp.concatenate(mixed, axis=1), go[...]).astype(BF)
        for s in range(4):
            GP[k, s % 2, s // 2] = part[:, s * W:(s + 1) * W]
        g_core(k).start()

    def g_reduce(k):
        g_core(k).wait_recv()
        GS[k] = (GP[k, c, 1 - y].astype(F32) + GR[k, 1 - y].astype(F32)).astype(BF)
        g_y(k).start()
        GOWN[k] = GP[k, c, y].astype(F32) + GR[k, y].astype(F32)

    order = (2, 1, 3, 0)
    for t, k in enumerate(order):
        mix(k)
        if t > 0:
            g_reduce(order[t - 1])
    g_reduce(order[-1])
    for k in order:
        g_y(k).wait_recv()
        final = (HL[k] + (GOWN[k] + GY[k].astype(F32))).astype(BF)
        if k:
            FB[k] = final
            g_z(k).start()
        else:
            RB[0] = final

    def placed(k, j):
        w = weight(ids_ref[B + j:B + j + 1], IDR[k][0:B])
        return wide(w, W) * RB[k].astype(F32)

    for j in range(B):
        OF[j] = placed(0, j)
    for k in order[:-2]:
        g_z(k).wait_recv()
        for j in range(B):
            OF[j] += placed(k, j)
    g_z(order[-2]).wait_recv()
    for j in range(B):
        out_ref[j * BLOCK:(j + 1) * BLOCK] = (OF[j] + placed(order[-2], j)).astype(BF)

    for k in range(3):
        x_y(k).wait_send()
    for k in range(4):
        x_core(k).wait_send()
        x_fwd(k).wait_send()

    @pl.when(me < N - 1)
    def _():
        halo_up.wait_send()

    @pl.when(me > 0)
    def _():
        halo_down.wait_send()
        halo_far.wait_send()

    for k in range(1, L):
        id_copy(k).wait_send()
        g_z(k).wait_send()
    for b in range(B):
        l_core(b).wait_send()
        l_y(b).wait_send()
        l_hid(b).wait_send()
        g_core(b).wait_send()
        g_y(b).wait_send()

    @pl.loop(1, N)
    def _(d):
        rs_copy(d).wait_send()
        ag_copy(d).wait_send()


def body(
    N, nodes_in, local_gain, w1, local_out, global_gain, w2, global_out, feature_map,
    neighbour_count, neighbour_blocks, metis_order, hashed_order,
):
    rows, W = nodes_in.shape
    B = metis_order.shape[0]
    SLOTS = neighbour_blocks.shape[1]
    D = w1.shape[1]
    SR = feature_map.shape[0] * feature_map.shape[2]
    vm = pl.BlockSpec(memory_space=pltpu.VMEM)
    hb = pl.BlockSpec(memory_space=pl.ANY)

    def V(*shape, dtype=BF):
        return pltpu.VMEM(shape, dtype)

    half = rows // 2
    S = pltpu.SemaphoreType.DMA
    scratch = [
        V(rows, W), V(1, D, dtype=F32), V(1, D, dtype=F32), V(*feature_map.shape),
        pltpu.SMEM((B,), jnp.int32), pltpu.SMEM((B, SLOTS), jnp.int32),
        pltpu.SMEM((B,), jnp.int32), pltpu.SMEM((B,), jnp.int32),
        V(2 * B, 128, dtype=jnp.int32), V(B, BLOCK, W, dtype=F32),
        V(3, D, W), V(W, D), V(3, D, W), V(W, D),
        V(2, 2, 4, half, W), V(2 * B, BLOCK, W), V(2 * B, BLOCK, W), V(B, BLOCK, W),
        V(W // 128, 128, 256), V(4, 2 * B, 128, dtype=jnp.int32),
        V(B, 2, 2, BLOCK, W), V(B, 2, BLOCK, W), V(B, 2, BLOCK, W), V(B, 2, BLOCK, W),
        V(B, 2, 2, BLOCK, W), V(B, BLOCK, 2 * W), V(SR, 128, dtype=F32),
        V(N, SR // N, 128), V(N, SR // N, 128), V(N, SR // N, 128),
        V(4, BLOCK, 2 * W), V(4, BLOCK, W, dtype=F32),
        V(4, 2, 2, BLOCK, W), V(4, 2, BLOCK, W), V(4, BLOCK, W), V(4, BLOCK, W, dtype=F32),
        V(4, BLOCK, W), V(4, BLOCK, W), V(4, BLOCK, W),
        S((8,)), S((4,)),
    ] + [S((4,))] * 6 + [S((3,))] * 2 + [S((4,))] * 2 + [S((4,))] * 6 + [S((N,))] * 4 + [S((4,))] * 6
    return pl.pallas_call(
        functools.partial(kernel, N, B, SLOTS),
        out_shape=jax.ShapeDtypeStruct((rows, W), BF),
        in_specs=[hb] * 12,
        out_specs=vm,
        scratch_shapes=scratch,
        compiler_params=pltpu.CompilerParams(
            collective_id=0, has_side_effects=True, vmem_limit_bytes=67043328),
        name="graph_pair",
    )(nodes_in, local_gain.reshape(1, D), w1, local_out, global_gain.reshape(1, D), w2, global_out,
      feature_map, neighbour_count, neighbour_blocks, metis_order, hashed_order)


def solution(mesh):
    in_specs = (
        P("nodes", "heads"), P(), P(None, None, "heads"), P("heads", None), P(),
        P(None, None, "heads"), P("heads", None), P("heads", None, None),
        P("nodes"), P("nodes", None), P("nodes"), P("nodes"),
    )
    return jax.shard_map(
        functools.partial(body, mesh.shape["nodes"]), mesh=mesh, in_specs=in_specs,
        out_specs=P("nodes", "heads"), check_vma=False)
```
